512 devices in a mesh: dp: 4 (over z_hi, core), blk: 32 (over z_lo, y), head: 4 (over x).
Axes of the slice: x: 4, y: 8, z: 8 (z_hi: 2, z_lo: 4; z = z_hi * 4 + z_lo), core: 2. Of those that a mesh axis runs over, the one named last changes fastest.
Arguments:
- queries: bfloat16 [4, 16384, 1024], P('dp', ('blk', 'head')), may hold values from -40 to 40
- keys_values: bfloat16 [4, 16384, 512], P('dp', ('blk', 'head')), may hold values from -40 to 40
- out_weight: bfloat16 [1024, 2048], P('head'), may hold values from -0.125 to 0.125
- cotangent: bfloat16 [4, 16384, 2048], P('dp', ('blk', 'head')), may hold values from -6 to 6
- passage_lengths: int32 [4, 32], P('dp'), may hold values from 1 to 1024, 15872 in all within a row
- causal_flags: int32 [4, 32], P('dp'), may hold values from 0 to 1
Outputs:
- attn: bfloat16 [4, 16384, 1024], P('dp', 'blk', 'head')
- grad_queries: bfloat16 [4, 16384, 1024], P('dp', 'blk', 'head')
- grad_keys_values: bfloat16 [4, 16384, 512], P('dp', 'blk', 'head')
- grad_out_weight: bfloat16 [1024, 2048], P('head')
The draws below stay inside these ranges and needn't reach their ends.
Inputs may be any that keep to these rules, and one draw needn't show every extreme that they name: `passage_lengths`: each row sums to 15872; its largest entry is 1024.
All inputs are finite; a program needn't handle non-finite values.
Results may differ from the reference program's by a relative error of at most 0.019.
Values may be sent and summed in bfloat16 or wider, within the bound.
No kernel may reach another device: no remote copies, remote signals or barrier semaphores. Data moves between devices by JAX's collectives and lax.ppermute only.
A program may use at most 128 MiB of HBM per device.

```python
import math
import jax
import jax.numpy as jnp
import numpy as np
from jax import lax

D = 2048
QUERY_HEADS = 16
KEY_VALUE_HEADS = 4
HEAD_SIZE = 64
LISTS = 32
GROUPS = 4
SEQUENCE_LENGTH = 16384
PREFIX = 512
MOST = 1024
N_BLK = 32


def draw_group(key):
    heads_per_group = QUERY_HEADS // KEY_VALUE_HEADS
    queries = jnp.clip(jax.random.normal(jax.random.fold_in(key, 101), (SEQUENCE_LENGTH, KEY_VALUE_HEADS, heads_per_group, HEAD_SIZE), jnp.float32), -5.0, 5.0)
    index_pairs = jnp.clip(jax.random.normal(jax.random.fold_in(key, 102), (SEQUENCE_LENGTH, KEY_VALUE_HEADS, 2 * HEAD_SIZE), jnp.float32), -5.0, 5.0)
    queries = jnp.clip(queries, -40.0, 40.0).reshape(SEQUENCE_LENGTH, QUERY_HEADS * HEAD_SIZE)
    index_pairs = jnp.clip(index_pairs, -40.0, 40.0).reshape(SEQUENCE_LENGTH, KEY_VALUE_HEADS * 2 * HEAD_SIZE)
    return (queries, index_pairs)


def draw_queries(key, part):
    drawn = jax.vmap(lambda index: draw_group(jax.random.fold_in(key, index))[0])(jnp.arange(GROUPS))
    return drawn.astype(jnp.bfloat16)


def draw_keys_values(key, part):
    drawn = jax.vmap(lambda index: draw_group(jax.random.fold_in(key, index))[1])(jnp.arange(GROUPS))
    return drawn.astype(jnp.bfloat16)


def place_ends(entries, rng, least, high):
    shape = entries.shape
    place = [jax.random.randint(jax.random.fold_in(rng, axis), (), 0, shape[axis]) for axis in range(len(shape))]
    entries = entries.at[tuple(place)].set(least)
    longest = shape.index(max(shape))
    place[longest] = (place[longest] + 1) % shape[longest]
    return entries.at[tuple(place)].set(high)


def levels(key, extent, split, smallest, high):
    factor_of, own = 1.0, jax.random.fold_in(key, 6)
    for axis_at, parts in split:
        heights = jnp.exp(jax.random.uniform(jax.random.fold_in(own, axis_at), (parts,), jnp.float32, smallest / len(split), high / len(split)))
        factor_of = factor_of * jnp.repeat(heights, extent[axis_at] // parts).reshape([-1 if axis == axis_at else 1 for axis in range(len(extent))])
    return factor_of


def profile(number_of, total, most, skew):
    portions = [(1 << 20) // math.isqrt(grade ** skew) + 1 for grade in range(2, number_of + 1)]
    spare, given = total - most - (number_of - 1), [1] * (number_of - 1)
    while spare > 0:
        candidates = [i for i in range(number_of - 1) if given[i] < most]
        pool, left = sum([portions[i] for i in candidates]), spare
        for i in candidates:
            addition = min(most - given[i], max(1, left * portions[i] // pool), spare)
            given[i] = given[i] + addition
            spare = spare - addition
    return np.array([most] + given)


def ragged_sizes(rng, number_of, total, limit, lean):
    if number_of == 2:
        one = jax.random.randint(rng, (), max(1, total - limit), min(limit, total - 1) + 1)
        return jnp.stack([one, total - one])
    sizes = jnp.asarray(profile(number_of, total, limit, lean), jnp.int32)
    couples = (number_of - 1) // 2
    giver, taker = sizes[1:1 + 2 * couples:2], sizes[2:2 + 2 * couples:2]
    margin = jnp.minimum(giver - 1, limit - taker)
    shifted = jax.random.randint(jax.random.fold_in(rng, 1), (couples,), 0, 1 << 20) % (margin + 1)
    sizes = sizes.at[1:1 + 2 * couples:2].set(giver - shifted).at[2:2 + 2 * couples:2].set(taker + shifted)
    return sizes[jax.random.permutation(jax.random.fold_in(rng, 2), number_of)]


def scatter_about(stream_key, dims, spread, most, pieces=(), kind=jnp.bfloat16):
    values = spread * jax.random.normal(stream_key, dims, jnp.float32)
    if pieces:
        values = values * levels(stream_key, dims, pieces, -0.22, 0.18)
    return jnp.clip(values, -most, most).astype(kind)


def setup_inputs(seed: int = 0) -> dict:
    splits = jax.random.split(jax.random.key(seed), 7)
    queries = draw_queries(jax.random.fold_in(splits[6], 71), 0)
    keys_values = draw_keys_values(jax.random.fold_in(splits[6], 71), 0)
    out_weight = scatter_about(splits[2], (QUERY_HEADS * HEAD_SIZE, D), D ** -0.5, 0.125, ((0, 4),))
    cotangent = scatter_about(splits[3], (GROUPS, SEQUENCE_LENGTH, D), 1.0, 6.0, ((0, 4), (1, 128)))
    passage_lengths = jax.vmap(lambda own: ragged_sizes(own, LISTS, SEQUENCE_LENGTH - PREFIX, MOST, 2))(jax.random.split(splits[4], GROUPS)).reshape((GROUPS, LISTS)).astype(jnp.int32)
    causal_flags = place_ends(jax.random.randint(splits[5], (GROUPS, LISTS), 0, 2), jax.random.fold_in(splits[5], 1), 0, 1).astype(jnp.int32)
    return dict(queries=queries, keys_values=keys_values, out_weight=out_weight, cotangent=cotangent, passage_lengths=passage_lengths, causal_flags=causal_flags)


neg_fill = -1.0e30


def rounded(values):
    return lax.optimization_barrier(values.astype(jnp.bfloat16)).astype(jnp.float32)


def describe(lengths, causal, positions, prefix):
    lengths = lengths.astype(jnp.int32)
    starts = (prefix + jnp.cumsum(lengths) - lengths).astype(jnp.int32)
    segment_id = jnp.sum((starts[None, :] <= positions[:, None]).astype(jnp.int32), axis=1).astype(jnp.int32)
    labels = jnp.arange(1, lengths.shape[0] + 1, dtype=jnp.int32)
    flag_of = jnp.sum(jnp.where(segment_id[:, None] == labels[None, :], causal[None, :], 0), axis=1).astype(jnp.int32)
    flag_of = flag_of + (segment_id == 0).astype(jnp.int32)
    return segment_id, flag_of


def permitted(query_info, key_info, query_pos, key_pos):
    query_seg, query_flag = query_info
    key_seg, key_flag = key_info
    same_list = query_seg[:, None] == key_seg[None, :]
    visible = same_list | (key_seg[None, :] == 0)
    ordered = (key_pos[None, :] <= query_pos[:, None]) | ((query_flag[:, None] == 0) & same_list)
    return visible & ordered


def reference(queries, keys_values, out_weight, cotangent, passage_lengths, causal_flags):
    block_rows = SEQUENCE_LENGTH // N_BLK
    window = block_rows + 2 * MOST
    heads_per_group = QUERY_HEADS // KEY_VALUE_HEADS
    scale = HEAD_SIZE ** -0.5

    def one_group(operands):
        grouped_query, grouped_key_value, group_dy, lengths, causal = operands
        query_head_list = grouped_query.reshape(SEQUENCE_LENGTH, KEY_VALUE_HEADS, heads_per_group, HEAD_SIZE)
        key_value_head_list = grouped_key_value.reshape(SEQUENCE_LENGTH, KEY_VALUE_HEADS, 2 * HEAD_SIZE)
        attention_gradient = jnp.dot(group_dy, out_weight.T, preferred_element_type=jnp.float32).astype(jnp.bfloat16)
        head_gradients = attention_gradient.reshape(SEQUENCE_LENGTH, KEY_VALUE_HEADS, heads_per_group, HEAD_SIZE)

        def prepare(index):
            first_row = (index * block_rows).astype(jnp.int32)
            query_pos = first_row + jnp.arange(block_rows, dtype=jnp.int32)
            begin = jnp.clip(first_row - MOST, PREFIX, SEQUENCE_LENGTH - window).astype(jnp.int32)
            key_pos = jnp.concatenate([jnp.arange(PREFIX, dtype=jnp.int32), begin + jnp.arange(window, dtype=jnp.int32)])
            chosen = jnp.concatenate([key_value_head_list[:PREFIX], lax.dynamic_slice_in_dim(key_value_head_list, begin, window, 0)], axis=0)
            allowed = permitted(describe(lengths, causal, query_pos, PREFIX), describe(lengths, causal, key_pos, PREFIX), query_pos, key_pos)
            q_block = lax.dynamic_slice_in_dim(query_head_list, first_row, block_rows, 0).astype(jnp.float32)
            key_part = chosen[:, :, :HEAD_SIZE].astype(jnp.float32)
            value_part = chosen[:, :, HEAD_SIZE:].astype(jnp.float32)
            scores = jnp.einsum("qgrd,kgd->qgrk", q_block, key_part) * scale
            return first_row, begin, allowed[:, None, None, :], q_block, key_part, value_part, scores

        def forward(index):
            first_row, begin, allowed, q_block, key_part, value_part, scores = prepare(index)
            running_max = jnp.max(jnp.where(allowed, scores, neg_fill), axis=-1)
            totals = jnp.sum(jnp.where(allowed, jnp.exp(scores - running_max[..., None]), 0.0), axis=-1)
            log_norm = running_max + jnp.log(totals)
            probs = jnp.where(allowed, jnp.exp(scores - log_norm[..., None]), 0.0)
            result = jnp.einsum("qgrk,kgd->qgrd", rounded(probs), value_part).astype(jnp.bfloat16)
            return result, log_norm

        output_list, norm_values = lax.map(forward, jnp.arange(N_BLK, dtype=jnp.int32))
        attn = output_list.reshape(SEQUENCE_LENGTH, QUERY_HEADS * HEAD_SIZE)
        attention_per_head = output_list.reshape(SEQUENCE_LENGTH, KEY_VALUE_HEADS, heads_per_group, HEAD_SIZE)
        norm_total_rows = norm_values.reshape(SEQUENCE_LENGTH, KEY_VALUE_HEADS, heads_per_group)
        weight_gradient = jnp.dot(attn.T, group_dy, preferred_element_type=jnp.float32)

        def backward_pass(key_value_gradient, index):
            first_row, begin, allowed, q_block, key_part, value_part, scores = prepare(index)
            log_norm = lax.dynamic_slice_in_dim(norm_total_rows, first_row, block_rows, 0)
            probs = jnp.where(allowed, jnp.exp(scores - log_norm[..., None]), 0.0)
            out_block = lax.dynamic_slice_in_dim(attention_per_head, first_row, block_rows, 0).astype(jnp.float32)
            d_block = lax.dynamic_slice_in_dim(head_gradients, first_row, block_rows, 0).astype(jnp.float32)
            row_dot = jnp.sum(d_block * out_block, axis=-1)
            dprob = jnp.einsum("qgrd,kgd->qgrk", d_block, value_part)
            dscore = rounded(probs * (dprob - row_dot[..., None]))
            grad_q = (scale * jnp.einsum("qgrk,kgd->qgrd", dscore, key_part)).astype(jnp.bfloat16)
            grad_k = scale * jnp.einsum("qgrk,qgrd->kgd", dscore, q_block)
            grad_v = jnp.einsum("qgrk,qgrd->kgd", rounded(probs), d_block)
            both = jnp.concatenate([grad_k, grad_v], axis=-1)
            key_value_gradient = key_value_gradient.at[:PREFIX].add(both[:PREFIX])
            current = lax.dynamic_slice_in_dim(key_value_gradient, begin, window, 0)
            key_value_gradient = lax.dynamic_update_slice_in_dim(key_value_gradient, current + both[PREFIX:], begin, 0)
            return key_value_gradient, grad_q

        key_value_gradient, query_gradients = lax.scan(backward_pass, jnp.zeros((SEQUENCE_LENGTH, KEY_VALUE_HEADS, 2 * HEAD_SIZE), jnp.float32), jnp.arange(N_BLK, dtype=jnp.int32))
        return attn, query_gradients.reshape(SEQUENCE_LENGTH, QUERY_HEADS * HEAD_SIZE), key_value_gradient.reshape(SEQUENCE_LENGTH, KEY_VALUE_HEADS * 2 * HEAD_SIZE).astype(jnp.bfloat16), weight_gradient

    attn, grad_q, key_value_gradient, weight_gradient = lax.map(one_group, (queries, keys_values, cotangent, passage_lengths, causal_flags))
    return attn, grad_q, key_value_gradient, jnp.sum(weight_gradient, axis=0).astype(jnp.bfloat16)
```

```python
import jax
import jax.numpy as jnp
from jax import lax
from jax.experimental import pallas as pl
from jax.experimental.pallas import tpu as pltpu
from jax.sharding import Mesh
from jax.sharding import PartitionSpec as P

LOG2E = 1.4426950408889634
LN2 = 0.6931471805599453
FILL = -1e30
FLOOR = -1e20
FAR = 1e9
TILE = 256
F32 = jnp.float32
BF16 = jnp.bfloat16


def exchange(pieces, axis):
    return lax.all_to_all(pieces, axis, 0, 0, tiled=True)


def copies(shard, axis):
    size = lax.axis_size(axis)
    return exchange(jnp.broadcast_to(shard[None], (size, *shard.shape)), axis)


def summed(pieces):
    return pieces.astype(F32).sum(axis=0)


def passed_along(value, axis, steps):
    count = lax.axis_size(axis)
    first, last = (max(0, -steps), min(count, count - steps))
    return lax.ppermute(value, axis, [(source, source + steps) for source in range(first, last)])


def from_first(value, near, nz, ny):
    own = lax.axis_index(near)
    rounds = (
        [[((0, 0), (0, d))] for d in (ny // 2, ny // 4, 3 * ny // 4)],
        [
            [((0, e), (dz, e + dy)) for e in range(0, ny, ny // 4)]
            for dz, dy in ((0, 1), (nz // 2, 0), (nz // 2, 1))
        ],
        [[((s, e), (s + 1, e)) for s in range(0, nz, nz // 2) for e in range(ny)]],
    )
    for moves in rounds:
        reached = []
        for move in moves:
            got = lax.ppermute(
                value, near, [(a * ny + b, c * ny + d) for (a, b), (c, d) in move]
            )
            reached.append(([c * ny + d for _, (c, d) in move], got))
        for targets, got in reached:
            hit = jnp.any(own == jnp.array(targets, jnp.int32))
            value = jnp.where(hit, got, value)
    return value


def dot(a, b, ca, cb):
    return lax.dot_general(a, b, (((ca,), (cb,)), ((), ())), preferred_element_type=F32)


def row_info(own, rows, prefix, lists, lengths_ref, flags_ref, lo_ref, hi_ref, span_ref):
    first = own * rows
    pos = (first + lax.broadcasted_iota(jnp.int32, (1, rows), 1)).astype(jnp.int32)
    tiles = rows // TILE

    def step(i, carry):
        start, lo, hi, spans = carry
        end = start + lengths_ref[0, i]
        flag = flags_ref[0, i]
        here = pos >= start
        causal = flag == 1
        lo = jnp.where(here, start, lo)
        hi = jnp.where(here, jnp.where(causal, pos, end - 1), hi)
        out = []
        for k in range(tiles):
            a, z = spans[k]
            t0 = first + k * TILE
            t1 = t0 + TILE - 1
            a = jnp.where(t0 >= start, start, a)
            z = jnp.where(t1 >= start, jnp.where(causal, t1, end - 1), z)
            out.append((a, z))
        return (end, lo, hi, tuple(out))

    none = jnp.int32(0)
    state = (
        jnp.int32(prefix),
        jnp.full((1, rows), 1 << 20, jnp.int32),
        jnp.full((1, rows), -1, jnp.int32),
        tuple((jnp.int32(prefix), none) for _ in range(tiles)),
    )
    _, lo, hi, spans = lax.fori_loop(0, lists, step, state)
    lo_ref[...] = lo.astype(F32)
    hi_ref[...] = hi.astype(F32)
    for k in range(tiles):
        span_ref[2 * k] = spans[k][0]
        span_ref[2 * k + 1] = spans[k][1]


def halves(kv):
    lane = lax.broadcasted_iota(jnp.int32, kv.shape, 1)
    low = lane < 64
    wide = kv.astype(F32)
    turned = pltpu.roll(wide, 64, 1)
    zero = jnp.zeros_like(wide)
    return [
        jnp.where(low, wide, zero).astype(BF16),
        jnp.where(low, zero, turned).astype(BF16),
        jnp.where(low, turned, zero).astype(BF16),
        jnp.where(low, zero, wide).astype(BF16),
    ]


def fill_window(blocks, rows, refs):
    for i, block in enumerate(blocks):
        for ref, part in zip(refs, halves(block[...])):
            ref[i * rows : (i + 1) * rows, :] = part


def tile_range(span_ref, k, base, last):
    a, z = span_ref[2 * k], span_ref[2 * k + 1]
    lo = jnp.clip(lax.shift_right_arithmetic(a - base, 8), 0, last)
    hi = jnp.clip(lax.shift_right_arithmetic(z - base, 8) + 1, 0, last)
    return lo, jnp.where(z >= a, hi, lo)


def forward_kernel(
    own_ref, lengths_ref, flags_ref, q_ref, m2, m1, here, p1, p2, pre,
    attn_ref, norm_ref,
    ke, ko, ve, vo, lo_ref, hi_ref, span_ref, lo_col, hi_col, m_ref, l_ref, acc_ref,
):
    rows = q_ref.shape[0]
    lists = lengths_ref.shape[1]
    prefix = pre.shape[0]
    own = own_ref[0]
    row_info(own, rows, prefix, lists, lengths_ref, flags_ref, lo_ref, hi_ref, span_ref)
    fill_window((m2, m1, here, p1, p2, pre), rows, (ke, ko, ve, vo))
    window = 5 * rows // TILE
    base = (own - 2) * rows
    scale2 = 0.125 * LOG2E
    lane = lax.broadcasted_iota(jnp.int32, (TILE, 128), 1)
    low = lane < 64
    lo_col[...] = jnp.transpose(jnp.broadcast_to(lo_ref[...], (128, rows)))
    hi_col[...] = jnp.transpose(jnp.broadcast_to(hi_ref[...], (128, rows)))
    for k in range(rows // TILE):
        at = slice(k * TILE, (k + 1) * TILE)
        m_ref[...] = jnp.full(m_ref.shape, FLOOR, F32)
        l_ref[...] = jnp.zeros(l_ref.shape, F32)
        acc_ref[...] = jnp.zeros(acc_ref.shape, F32)
        pairs = (q_ref[at, 0:128], q_ref[at, 128:256])
        own_pos = ((own * rows + k * TILE) + lax.broadcasted_iota(jnp.int32, (TILE, 128), 0)).astype(F32)

        def visit(j, first_key, lo, hi):
            span = pl.ds(pl.multiple_of(j * TILE, TILE), TILE)
            key_pos = (first_key + lax.broadcasted_iota(jnp.int32, (TILE, TILE), 1)).astype(F32)
            lo2 = jnp.concatenate([lo, lo], axis=1)
            hi2 = jnp.concatenate([hi, hi], axis=1)
            seen = (key_pos >= lo2) & (key_pos <= hi2)
            kk = (ke[span, :], ko[span, :])
            vv = jnp.concatenate([ve[span, :], vo[span, :]], axis=0)
            for pair in range(2):
                probs, factors = [], []
                for odd in range(2):
                    r = 2 * pair + odd
                    s = dot(pairs[pair], kk[odd], 1, 1) * scale2
                    s = jnp.where(seen, s, FILL)
                    best = m_ref[r]
                    new = jnp.maximum(best, jnp.max(s, axis=1, keepdims=True))
                    p = jnp.exp2(s - jnp.concatenate([new, new], axis=1))
                    factor = jnp.exp2(best - new)
                    l_ref[r] = l_ref[r] * factor + jnp.sum(p, axis=1, keepdims=True)
                    m_ref[r] = new
                    probs.append(p.astype(BF16))
                    factors.append(factor)
                part = dot(jnp.concatenate(probs, axis=1), vv, 1, 0)
                acc_ref[pair] = acc_ref[pair] * jnp.where(low, factors[0], factors[1]) + part

        start, stop = tile_range(span_ref, k, base, window)

        def near(j, _):
            visit(j, base + j * TILE, lo_col[at, :], hi_col[at, :])
            return 0

        lax.fori_loop(start, stop, near, 0)

        def far(j, _):
            visit(window + j, j * TILE, jnp.full((TILE, 128), -1.0, F32), own_pos)
            return 0

        lax.fori_loop(0, prefix // TILE, far, 0)
        norms = jnp.zeros((TILE, 128), F32)
        for pair in range(2):
            e, o = 2 * pair, 2 * pair + 1
            total = jnp.where(low, l_ref[e], l_ref[o])
            attn_ref[at, pair * 128 : (pair + 1) * 128] = (acc_ref[pair] / total).astype(BF16)
            for r in (e, o):
                norms = jnp.where(lane == r, m_ref[r] + jnp.log(l_ref[r]) * LOG2E, norms)
        norm_ref[:, at] = jnp.transpose(norms)[:8]


def backward_kernel(
    own_ref, lengths_ref, flags_ref, q_ref, d_ref, attn_ref, norm_ref, m2, m1, here, p1, p2, pre,
    gq_ref, gm2, gm1, ghere, gp1, gp2, gpre,
    ke, ko, ve, vo, lo_ref, hi_ref, span_ref, dot_ref, stack_ref, gq_acc, gkv_acc,
):
    rows = q_ref.shape[0]
    lists = lengths_ref.shape[1]
    prefix = pre.shape[0]
    own = own_ref[0]
    row_info(own, rows, prefix, lists, lengths_ref, flags_ref, lo_ref, hi_ref, span_ref)
    fill_window((m2, m1, here, p1, p2, pre), rows, (ke, ko, ve, vo))
    window = 5 * rows // TILE
    base = (own - 2) * rows
    scale2 = 0.125 * LOG2E
    product = d_ref[...].astype(F32) * attn_ref[...].astype(F32)
    turned = jnp.transpose(product)
    for r in range(4):
        dot_ref[r : r + 1, :] = jnp.sum(turned[r * 64 : (r + 1) * 64], axis=0, keepdims=True)
    low = lax.broadcasted_iota(jnp.int32, (rows, 128), 1) < 64
    zero = jnp.zeros((rows, 128), F32)
    for pair in range(2):
        cols = slice(pair * 128, (pair + 1) * 128)
        d = d_ref[:, cols].astype(F32)
        q = q_ref[:, cols].astype(F32)
        stack_ref[4 * pair + 0] = jnp.where(low, zero, pltpu.roll(d, 64, 1)).astype(BF16)
        stack_ref[4 * pair + 1] = jnp.where(low, q, zero).astype(BF16)
        stack_ref[4 * pair + 2] = jnp.where(low, zero, d).astype(BF16)
        stack_ref[4 * pair + 3] = jnp.where(low, pltpu.roll(q, 64, 1), zero).astype(BF16)
    gkv_acc[...] = jnp.zeros(gkv_acc.shape, F32)
    gq_acc[...] = jnp.zeros(gq_acc.shape, F32)
    for k in range(rows // TILE):
        at = slice(k * TILE, (k + 1) * TILE)
        q_pairs = (q_ref[at, 0:128], q_ref[at, 128:256])
        d_pairs = (d_ref[at, 0:128], d_ref[at, 128:256])
        own_pos = ((own * rows + k * TILE) + lax.broadcasted_iota(jnp.int32, (1, TILE), 1)).astype(F32)

        def visit(j, first_key, lo, hi):
            span = pl.ds(pl.multiple_of(j * TILE, TILE), TILE)
            key_pos = (first_key + lax.broadcasted_iota(jnp.int32, (TILE, TILE), 0)).astype(F32)
            seen = (key_pos >= lo) & (key_pos <= hi)
            kk = (ke[span, :], ko[span, :])
            vv = (ve[span, :], vo[span, :])
            keys = jnp.concatenate(kk, axis=0)
            total = gkv_acc[span, :]
            for pair in range(2):
                scores = []
                for odd in range(2):
                    r = 2 * pair + odd
                    s = dot(kk[odd], q_pairs[pair], 1, 1) * scale2 - norm_ref[r : r + 1, at]
                    p = jnp.exp2(jnp.where(seen, s, FILL))
                    dp = dot(vv[odd], d_pairs[pair], 1, 1)
                    ds = (p * (dp - dot_ref[r : r + 1, at])).astype(BF16)
                    both = jnp.concatenate([p.astype(BF16), ds], axis=1)
                    side = jnp.concatenate([stack_ref[2 * r, at, :], stack_ref[2 * r + 1, at, :]], axis=0)
                    total = total + dot(both, side, 1, 0)
                    scores.append(ds)
                gq_acc[pair, at, :] += dot(jnp.concatenate(scores, axis=0), keys, 0, 0)
            gkv_acc[span, :] = total

        start, stop = tile_range(span_ref, k, base, window)

        def near(j, _):
            visit(j, base + j * TILE, lo_ref[:, at], hi_ref[:, at])
            return 0

        lax.fori_loop(start, stop, near, 0)

        def far(j, _):
            visit(window + j, j * TILE, jnp.full((1, TILE), -1.0, F32), own_pos)
            return 0

        lax.fori_loop(0, prefix // TILE, far, 0)
    for pair in range(2):
        gq_ref[:, pair * 128 : (pair + 1) * 128] = (gq_acc[pair] * 0.125).astype(BF16)
    factor = jnp.where(lax.broadcasted_iota(jnp.int32, (rows, 128), 1) < 64, 0.125, 1.0)
    for i, out in enumerate((gm2, gm1, ghere, gp1, gp2, gpre)):
        out[...] = (gkv_acc[i * rows : (i + 1) * rows, :] * factor).astype(out.dtype)


def kernel_specs(n_vmem):
    smem = pl.BlockSpec(memory_space=pltpu.SMEM)
    vmem = pl.BlockSpec(memory_space=pltpu.VMEM)
    return [smem] * 3 + [vmem] * n_vmem


def run_forward(own, lengths, flags, q, blocks):
    rows, width = q.shape
    vmem = pl.BlockSpec(memory_space=pltpu.VMEM)
    keys = 6 * rows
    return pl.pallas_call(
        forward_kernel,
        name="attn_forward",
        in_specs=kernel_specs(7),
        out_specs=(vmem, vmem),
        out_shape=(
            jax.ShapeDtypeStruct((rows, width), BF16),
            jax.ShapeDtypeStruct((8, rows), F32),
        ),
        scratch_shapes=[pltpu.VMEM((keys, 128), BF16)] * 4
        + [pltpu.VMEM((1, rows), F32)] * 2
        + [pltpu.SMEM((2 * (rows // TILE),), jnp.int32)]
        + [pltpu.VMEM((rows, 128), F32)] * 2
        + [pltpu.VMEM((4, TILE, 128), F32)] * 2
        + [pltpu.VMEM((2, TILE, 128), F32)],
        cost_estimate=pl.CostEstimate(flops=3 * 10**9, bytes_accessed=2 * 10**6, transcendentals=4 * 10**6),
    )(own, lengths, flags, q, *blocks)


def run_backward(own, lengths, flags, q, d, attn, norm, blocks):
    rows, width = q.shape
    vmem = pl.BlockSpec(memory_space=pltpu.VMEM)
    keys = 6 * rows
    side = jax.ShapeDtypeStruct((rows, 128), BF16)
    return pl.pallas_call(
        backward_kernel,
        name="attn_backward",
        in_specs=kernel_specs(10),
        out_specs=(vmem,) * 7,
        out_shape=(
            jax.ShapeDtypeStruct((rows, width), BF16),
            side, side, jax.ShapeDtypeStruct((rows, 128), F32), side, side, side,
        ),
        scratch_shapes=[pltpu.VMEM((keys, 128), BF16)] * 4
        + [pltpu.VMEM((1, rows), F32)] * 2
        + [pltpu.SMEM((2 * (rows // TILE),), jnp.int32)]
        + [pltpu.VMEM((8, rows), F32), pltpu.VMEM((8, rows, 128), BF16)]
        + [pltpu.VMEM((2, rows, 128), F32), pltpu.VMEM((keys, 128), F32)],
        cost_estimate=pl.CostEstimate(flops=6 * 10**9, bytes_accessed=3 * 10**6, transcendentals=4 * 10**6),
    )(own, lengths, flags, q, d, attn, norm, *blocks)


def on_device(queries, keys_values, out_weight, cotangent, passage_lengths, causal_flags):
    heads = lax.axis_size("x")
    near = ("zl", "y")
    own = lax.axis_index(near)
    part = queries.shape[1]
    rows = part * heads
    joined = jnp.concatenate(
        [queries[0].reshape(part, heads, -1), keys_values[0].reshape(part, heads, -1)], axis=2
    )
    arrived = exchange(jnp.moveaxis(joined, 1, 0), "x").reshape(rows, -1)
    width = queries.shape[2] // heads
    q, kv = arrived[:, :width], arrived[:, width:]
    shard_rows = copies(cotangent[0], "x").reshape(rows, -1)
    ny, nz = lax.axis_size("y"), lax.axis_size("zl")
    instruction = from_first(kv, near, nz, ny)
    moves = (2, 1, -1, -2)
    m2, m1, p1, p2 = (passed_along(kv, near, m) for m in moves)
    blocks = (m2, m1, kv, p1, p2, instruction)
    index = own.astype(jnp.int32).reshape(1)
    attn, norm = run_forward(index, passage_lengths, causal_flags, q, blocks)
    weight_acc = dot(attn, shard_rows, 0, 0).astype(BF16)
    product = dot(shard_rows, out_weight, 1, 1).astype(BF16)
    half = weight_acc.shape[0] // 2
    share = summed(exchange(weight_acc.reshape(2, half, -1), "c")).astype(BF16)
    grad_q, g2, g1, g_own, g_1, g_2, g_pre = run_backward(
        index, passage_lengths, causal_flags, q, product, attn, norm, blocks
    )
    plane = ("zh", "zl", "y")
    members = lax.axis_size(plane)
    share = summed(exchange(share.reshape(members, half // members, -1), plane)).astype(BF16)
    share = copies(share, plane).reshape(half, -1)
    grad_weight = copies(share, "c").reshape(2 * half, -1)
    total = summed(exchange(g_pre.reshape(ny, rows // ny, -1), "y")).astype(BF16)
    total = summed(copies(total, "zl")).astype(BF16)
    total = copies(total, "y").reshape(rows, -1).astype(F32)
    for value, m in zip((g2, g1, g_1, g_2), moves):
        g_own = g_own + passed_along(value, near, -m).astype(F32)
    g_own = g_own + jnp.where(own == 0, total, 0.0)
    return (attn[None], grad_q[None], g_own.astype(BF16)[None], grad_weight)


def solution(mesh):
    fine = Mesh(mesh.devices.reshape(2, 2, 4, 8, 4), ("zh", "c", "zl", "y", "x"))
    dp, blk, head = ("zh", "c"), ("zl", "y"), "x"
    return jax.shard_map(
        on_device,
        mesh=fine,
        in_specs=(
            P(dp, (*blk, head), None),
            P(dp, (*blk, head), None),
            P(head, None),
            P(dp, (*blk, head), None),
            P(dp, None),
            P(dp, None),
        ),
        out_specs=(
            P(dp, blk, head),
            P(dp, blk, head),
            P(dp, blk, head),
            P(head, None),
        ),
        check_vma=False,
    )
```
